32 devices in a mesh: gx: 4 (over x, core), yz: 8 (over z, y).
Axes of the slice: x: 2, y: 2, z: 4, core: 2. Of those that a mesh axis runs over, the one named last changes fastest.
Arguments:
- pressure: bfloat16 [8192, 4096], P(('gx', 'yz')), may hold values from -6 to 6
- face_block: int32 [131072], P(('gx', 'yz')), may hold values from 0 to 255
- stencil_local: int32 [32, 131072], P(None, ('gx', 'yz')), may hold values from 0 to 4095
- stencil_weight: float32 [32, 131072], P(None, ('gx', 'yz')), may hold values from 0 to 0.25
- area_normal: float32 [12, 131072], P(None, ('gx', 'yz')), may hold values from -6 to 6
- face_part: int32 [131072, 1], P(('gx', 'yz')), may hold values from 0 to 31; in each aligned block of 4096 rows (0 to 4095, 4096 to 8191, ...) at most 256 rows name the same one
- face_nodes: int32 [8, 131072], P(None, ('gx', 'yz')), may hold values from 0 to 1023
- stiffness: float32 [60, 60, 8192], P(None, None, ('gx', 'yz')), may hold values from -0.075 to 6, as said below
- connect: int32 [20, 8192], P(None, ('gx', 'yz')), may hold values from 0 to 1279
- halo_nodes: int32 [2, 4096], P(None, ('gx', 'yz')), may hold values from 0 to 1023
- node_mass: float32 [32768], P(('gx', 'yz')), may hold values from 24 to 160
- displacement: float32 [3, 32768], P(None, ('gx', 'yz')), may hold values from -6 to 6
- velocity: float32 [3, 32768], P(None, ('gx', 'yz')), may hold values from -3 to 3
Outputs:
- node_disp: float32 [3, 32768], P(None, ('gx', 'yz'))
- face_disp: float32 [12, 131072], P(None, ('gx', 'yz'))
The draws below stay inside these ranges and needn't reach their ends.
Inputs may be any that keep to these rules, and one draw needn't show every extreme that they name: `face_part`: the faces of one device name no partition more than 256 times; in every draw some device names some partition exactly 256 times. `connect`: local node l of a partition: l < 1024 is owned, 1024 + g is entry g of the previous partition's row 1, 1152 + g entry g of the next partition's row 0 (along gx+yz). `halo_nodes`: each partition's 128 entries of row 0 are owned nodes held as ghosts by the previous partition, row 1 by the next; entries may repeat. `stiffness`: each element's matrix is symmetric positive definite.
All inputs are finite; a program needn't handle non-finite values.
Results may differ from the reference program's by a relative error of at most 0.0003.
Values sent between devices are 32-bit elements; how exact they have to be, the bound alone decides.
A program may use at most 256 MiB of HBM per device.

```python
import math
import jax
import jax.numpy as jnp
import numpy as np
from jax import lax

BLK_DEV = 256
BLOCK = 4096
FACE_DEV = 4096
ELEM_DEV = 256
SUBSTEPS = 4
NODE_DEV = 1024
GHOST = 128
CAP = 256
BLOCKS = 8192
FACES = 131072
ELEMS = 8192
NODES = 32768
GHOSTS = 4096
N_GX = 4
N_YZ = 8


def draw_stiffness(key, part):
    raw_entries = jax.random.uniform(key, (60, 60, ELEMS), jnp.float32, -0.05, 0.05)
    symmetric = 0.5 * (raw_entries + jnp.transpose(raw_entries, (1, 0, 2)))
    diag_mask = jnp.eye(60, dtype=jnp.float32)[:, :, None]
    off_part = symmetric * (1.0 - diag_mask)
    diagonal = 1.25 * jnp.sum(jnp.abs(off_part), axis=1) + 0.25
    matrix = off_part + diag_mask * diagonal[:, None, :]
    return matrix


def plant(values, stream_key, low, high):
    dims = values.shape
    index_at = [jax.random.randint(jax.random.fold_in(stream_key, axis), (), 0, dims[axis]) for axis in range(len(dims))]
    values = values.at[tuple(index_at)].set(low)
    longest = dims.index(max(dims))
    index_at[longest] = (index_at[longest] + 1) % dims[longest]
    return values.at[tuple(index_at)].set(high)


def shard_levels(stream_key, dims, pieces, low, largest):
    loudness, own = 1.0, jax.random.fold_in(stream_key, 6)
    for axis_at, shards_of in pieces:
        steps = jnp.exp(jax.random.uniform(jax.random.fold_in(own, axis_at), (shards_of,), jnp.float32, low / len(pieces), largest / len(pieces)))
        loudness = loudness * jnp.repeat(steps, dims[axis_at] // shards_of).reshape([-1 if axis == axis_at else 1 for axis in range(len(dims))])
    return loudness


def routed_block(stream_key, own, number, rows, amount, top, reach, skew):
    sequence = jax.random.permutation(stream_key, amount)
    heavy_load, common = shares(amount, rows * top, reach, skew, True), shares(amount, rows * top, reach, skew, False)
    places = jnp.arange(amount)

    def named(tallies, turn):
        used = int((tallies > 0).sum())
        fixed = max(1, used // 4)
        passed = fixed + (places - fixed + turn * (used - fixed)) % max(1, amount - fixed)
        return jnp.zeros((amount,), jnp.int32).at[sequence[jnp.where(places < fixed, places, passed)]].set(jnp.asarray(tallies, jnp.int32))

    tallies = jnp.where(number % 4 == 0, named(heavy_load, number // 4), named(common, number - number // 4 - 1))
    mixed = jax.random.permutation(jax.random.fold_in(own, 3), amount)
    giver, sink = mixed[0:amount // 2 * 2:2], mixed[1:amount // 2 * 2:2]
    slack = jnp.minimum(tallies[giver] - 1, reach - tallies[sink]) // 2
    slack = jnp.where((giver == sequence[0]) | (sink == sequence[0]) | (tallies[sink] == 0), 0, jnp.maximum(slack, 0))
    passed = jax.random.randint(jax.random.fold_in(own, 4), (amount // 2,), 0, 1 << 20) % (slack + 1)
    tallies = tallies.at[giver].add(-passed).at[sink].add(passed)
    labels = jnp.searchsorted(jnp.cumsum(tallies), jnp.arange(rows * top), side="right").astype(jnp.int32)
    table = labels.reshape(top, rows).T
    table = table[jax.random.permutation(jax.random.fold_in(own, 1), rows)]
    turn = jax.random.randint(jax.random.fold_in(own, 2), (rows, 1), 0, top)
    return jnp.take_along_axis(table, (jnp.arange(top)[None, :] + turn) % top, axis=1)


def shares(number_of, total, most, skew, full):
    loads = [(1 << 20) // math.isqrt(rank ** skew) + 1 for rank in range(1, number_of + 1)]
    largest = most if full else min(most, max(-(-total // number_of), total * loads[0] // sum(loads)))
    least = 1 if total - largest >= number_of - 1 else 0
    given, spare = [largest] + [least] * (number_of - 1), total - largest - least * (number_of - 1)
    while spare > 0:
        candidates = [i for i in range(1, number_of) if given[i] < largest] or [i for i in range(1, number_of) if given[i] < most]
        whole, left = sum([loads[i] for i in candidates]), spare
        for i in candidates:
            extra = min(most - given[i], max(1, left * loads[i] // whole), spare)
            given[i] = given[i] + extra
            spare = spare - extra
    return np.array(given)


def centred(key, extent, width, reach, pieces=(), kind=jnp.bfloat16):
    loudness = shard_levels(key, extent, pieces, -0.22, 0.18) if pieces else 1.0
    values = jax.random.normal(key, extent, jnp.float32) * width * loudness
    return jnp.minimum(jnp.maximum(values, -reach), reach).astype(kind)


def setup_inputs(seed: int = 0) -> dict:
    streams_of = jax.random.split(jax.random.key(seed), 14)
    pressure = centred(streams_of[0], (BLOCKS, BLOCK), 1.0, 6.0, ((0, 32),))
    face_block = plant(jax.random.randint(streams_of[1], (FACES,), 0, BLK_DEV), jax.random.fold_in(streams_of[1], 1), 0, BLK_DEV - 1).astype(jnp.int32)
    stencil_local = plant(jax.random.randint(streams_of[2], (32, FACES), 0, BLOCK), jax.random.fold_in(streams_of[2], 1), 0, BLOCK - 1).astype(jnp.int32)
    stencil_weight = jnp.clip(0.25 * jax.random.uniform(streams_of[3], (32, FACES), jnp.float32) ** shard_levels(streams_of[3], (32, FACES), ((1, 32),), -0.2, 0.2), 0.0, 0.25)
    area_normal = centred(streams_of[4], (12, FACES), 1.0, 6.0, ((1, 32),), jnp.float32)
    face_part_keys = jax.random.split(jax.random.fold_in(streams_of[5], 1), FACES // FACE_DEV)
    face_part_turns = jax.random.permutation(jax.random.fold_in(streams_of[5], 3), FACES // FACE_DEV)
    face_part = jax.vmap(lambda own, number: routed_block(jax.random.fold_in(streams_of[5], 2), own, number, FACE_DEV, N_GX * N_YZ, 1, CAP, 2))(face_part_keys, face_part_turns).reshape((FACES, 1))
    face_nodes = plant(jax.random.randint(streams_of[6], (8, FACES), 0, NODE_DEV), jax.random.fold_in(streams_of[6], 1), 0, NODE_DEV - 1).astype(jnp.int32)
    stiffness = draw_stiffness(jax.random.fold_in(streams_of[13], 71), 0)
    connect = plant(jax.random.randint(streams_of[8], (20, ELEMS), 0, NODE_DEV + 2 * GHOST), jax.random.fold_in(streams_of[8], 1), 0, (NODE_DEV + 2 * GHOST) - 1).astype(jnp.int32)
    halo_nodes = plant(jax.random.randint(streams_of[9], (2, GHOSTS), 0, NODE_DEV), jax.random.fold_in(streams_of[9], 1), 0, NODE_DEV - 1).astype(jnp.int32)
    node_mass = jnp.clip(jnp.exp(math.log(160.0) - 1.89712 * jax.random.uniform(streams_of[10], (NODES,), jnp.float32) ** shard_levels(streams_of[10], (NODES,), ((0, 32),), -0.2, 0.2)), 24.0, 160.0)
    displacement = centred(streams_of[11], (3, NODES), 1.0, 6.0, ((1, 32),), jnp.float32)
    velocity = centred(streams_of[12], (3, NODES), 0.5, 3.0, ((1, 32),), jnp.float32)
    return dict(pressure=pressure, face_block=face_block, stencil_local=stencil_local, stencil_weight=stencil_weight, area_normal=area_normal, face_part=face_part, face_nodes=face_nodes, stiffness=stiffness, connect=connect, halo_nodes=halo_nodes, node_mass=node_mass, displacement=displacement, velocity=velocity)


def shape_table():
    corner_u = [-1, 1, 1, -1, 0, 1, 0, -1]
    corner_v = [-1, -1, 1, 1, -1, 0, 1, 0]
    gauss_point = 1.0 / math.sqrt(3.0)
    points = [(-gauss_point, -gauss_point), (gauss_point, -gauss_point), (gauss_point, gauss_point), (-gauss_point, gauss_point)]
    shape_values = np.zeros((4, 8), np.float32)
    for position, (coord_u, coord_v) in enumerate(points):
        for corner in range(8):
            node_u = corner_u[corner]
            node_v = corner_v[corner]
            if corner < 4:
                entry_value = 0.25 * (1 + coord_u * node_u) * (1 + coord_v * node_v) * (coord_u * node_u + coord_v * node_v - 1)
            elif node_u == 0:
                entry_value = 0.5 * (1 - coord_u * coord_u) * (1 + coord_v * node_v)
            else:
                entry_value = 0.5 * (1 + coord_u * node_u) * (1 - coord_v * coord_v)
            shape_values[position, corner] = entry_value
    return shape_values

def reference(pressure, face_block, stencil_local, stencil_weight, area_normal, face_part, face_nodes, stiffness, connect, halo_nodes, node_mass, displacement, velocity):
    highest = lax.Precision.HIGHEST
    devices = N_GX * N_YZ
    shapes = jnp.asarray(shape_table(), dtype=jnp.float32)
    faces = FACE_DEV * devices
    owner = jnp.arange(faces, dtype=jnp.int32) // FACE_DEV
    block_index = owner * BLK_DEV + face_block
    cell_index = block_index[None, :] * BLOCK + stencil_local
    cell_values = pressure.reshape(-1)[cell_index].astype(jnp.float32)
    face_pressure = lax.optimization_barrier(jnp.sum((stencil_weight * cell_values).reshape(4, 8, faces), axis=1))
    traction = -(area_normal.reshape(3, 4, faces) * face_pressure[None])
    face_global = face_part[:, 0][None, :] * NODE_DEV + face_nodes
    total_nodes = NODE_DEV * devices
    load = jnp.einsum('qa,cqf->caf', shapes, traction, precision=highest)
    external = jnp.zeros((3, total_nodes), jnp.float32).at[:, face_global.reshape(-1)].add(load.reshape(3, -1))
    span = NODE_DEV + 2 * GHOST
    device_ids = jnp.arange(devices, dtype=jnp.int32)[:, None]
    owned = device_ids * NODE_DEV + jnp.arange(NODE_DEV, dtype=jnp.int32)[None, :]
    halo_grid = halo_nodes.reshape(2, devices, GHOST)
    from_prev = jnp.where(device_ids >= 1, (device_ids - 1) * NODE_DEV + jnp.roll(halo_grid[1], 1, axis=0), total_nodes).astype(jnp.int32)
    from_next = jnp.where(device_ids < devices - 1, (device_ids + 1) * NODE_DEV + jnp.roll(halo_grid[0], -1, axis=0), total_nodes).astype(jnp.int32)
    local_global = jnp.concatenate([owned, from_prev, from_next], axis=1).reshape(-1)
    elem_owner = jnp.arange(ELEM_DEV * devices, dtype=jnp.int32) // ELEM_DEV
    element_global = local_global[elem_owner[None, :] * span + connect]
    flat_index = element_global.reshape(-1)
    node_disp = displacement
    node_vel = velocity
    for substep in range(SUBSTEPS):
        padded = jnp.concatenate([node_disp, jnp.zeros((3, 1), jnp.float32)], axis=1)
        element_disp = padded[:, element_global].reshape(60, -1)
        element_force = lax.map(lambda stiff_row: lax.optimization_barrier(jnp.sum(stiff_row * element_disp, axis=0)), stiffness)
        internal = jnp.zeros((3, total_nodes + 1), jnp.float32).at[:, flat_index].add(element_force.reshape(3, -1))[:, :total_nodes]
        node_vel = node_vel + (external - internal) / node_mass[None, :]
        node_disp = node_disp + node_vel
    gathered = node_disp[:, face_global]
    face_disp = jnp.einsum('qa,caf->cqf', shapes, gathered, precision=highest).reshape(12, faces)
    return (node_disp, face_disp)
```

```python
import math

import jax
import jax.numpy as jnp
import numpy as np
from jax import lax
from jax.experimental import pallas as pl
from jax.experimental.pallas import tpu as pltpu
from jax.sharding import PartitionSpec as P

SUBSTEPS = 4


def with_halo(cells, sides, width):
    for axis, dim in sides:
        count = lax.axis_size(axis)
        ends = count - 1
        head = lax.slice_in_dim(cells, 0, width, axis=dim)
        tail = lax.slice_in_dim(cells, cells.shape[dim] - width, cells.shape[dim], axis=dim)
        cells = jnp.concatenate(
            [
                lax.ppermute(tail, axis, [(i, (i + 1) % count) for i in range(ends)]),
                cells,
                lax.ppermute(head, axis, [((i + 1) % count, i) for i in range(ends)]),
            ],
            axis=dim,
        )
    return cells


def shape_table():
    corner_u = [-1, 1, 1, -1, 0, 1, 0, -1]
    corner_v = [-1, -1, 1, 1, -1, 0, 1, 0]
    gauss_point = 1.0 / math.sqrt(3.0)
    points = [
        (-gauss_point, -gauss_point),
        (gauss_point, -gauss_point),
        (gauss_point, gauss_point),
        (-gauss_point, gauss_point),
    ]
    shape_values = np.zeros((4, 8), np.float32)
    for position, (coord_u, coord_v) in enumerate(points):
        for corner in range(8):
            node_u = corner_u[corner]
            node_v = corner_v[corner]
            if corner < 4:
                entry_value = (
                    0.25
                    * (1 + coord_u * node_u)
                    * (1 + coord_v * node_v)
                    * (coord_u * node_u + coord_v * node_v - 1)
                )
            elif node_u == 0:
                entry_value = 0.5 * (1 - coord_u * coord_u) * (1 + coord_v * node_v)
            else:
                entry_value = 0.5 * (1 + coord_u * node_u) * (1 - coord_v * coord_v)
            shape_values[position, corner] = entry_value
    return shape_values


def hot_pair(indices, extent):
    lanes_width = 32
    upper_count = -(-extent // lanes_width)
    upper_hot = (
        indices[None, :] // lanes_width == lax.broadcasted_iota(jnp.int32, (upper_count, 1), 0)
    ).astype(jnp.float32)
    lower_hot = (
        indices[None, :] % lanes_width == lax.broadcasted_iota(jnp.int32, (lanes_width, 1), 0)
    ).astype(jnp.float32)
    return (upper_hot, lower_hot)


def pick_cols(table, hots):
    upper_hot, lower_hot = hots
    lanes_width = lower_hot.shape[0]
    upper_count = upper_hot.shape[0]
    comps, extent = table.shape
    grid = (
        table.reshape(comps, upper_count, lanes_width)
        .transpose(1, 0, 2)
        .reshape(upper_count, comps * lanes_width)
    )
    rows_out = lax.dot_general(
        grid,
        upper_hot,
        (((0,), (0,)), ((), ())),
        precision=lax.Precision.HIGHEST,
        preferred_element_type=jnp.float32,
    )
    return jnp.sum(rows_out.reshape(comps, lanes_width, -1) * lower_hot[None], axis=1)


def spread_cols(values, hots):
    upper_hot, lower_hot = hots
    lanes_width = lower_hot.shape[0]
    upper_count = upper_hot.shape[0]
    comps = values.shape[0]
    masked = (values[:, None, :] * lower_hot[None]).reshape(comps * lanes_width, -1)
    summed = lax.dot_general(
        masked,
        upper_hot,
        (((1,), (1,)), ((), ())),
        precision=lax.Precision.HIGHEST,
        preferred_element_type=jnp.float32,
    )
    return (
        summed.reshape(comps, lanes_width, upper_count)
        .transpose(0, 2, 1)
        .reshape(comps, upper_count * lanes_width)
    )


def arrival_order(target, devices):
    row_count = target.shape[0]
    group_rows = min(512, row_count)
    groups = row_count // group_rows
    onehot = (target[:, None] == jnp.arange(devices, dtype=jnp.int32)[None, :]).astype(jnp.bfloat16)
    onehot = onehot.reshape(groups, group_rows, devices)
    lower_ones = (
        lax.broadcasted_iota(jnp.int32, (group_rows, group_rows), 0)
        > lax.broadcasted_iota(jnp.int32, (group_rows, group_rows), 1)
    ).astype(jnp.bfloat16)
    before = jnp.einsum("ij,gjd->gid", lower_ones, onehot, preferred_element_type=jnp.float32)
    onehot_float = onehot.astype(jnp.float32)
    totals = jnp.sum(onehot_float, axis=1)
    offsets = jnp.cumsum(totals, axis=0) - totals
    placed = jnp.sum((before + offsets[:, None, :]) * onehot_float, axis=2)
    return placed.reshape(row_count).astype(jnp.int32)


LANES = 128
SUBLANES = 8


def gather_entries(hot, table, entries, rows_ref, low_ref, high_ref, value_ref):
    tile = hot.shape[0]
    entry_count = entries.shape[0]
    chunks = table.shape[1] // LANES
    rows_ref[...] = jnp.dot(hot, table, preferred_element_type=jnp.float32)
    padded = jnp.concatenate(
        [entries, jnp.zeros((LANES - entry_count, tile), jnp.int32)], axis=0
    ).T
    low_ref[...] = lax.rem(padded, LANES)
    high_ref[...] = lax.div(padded, LANES)

    def group(step, carry):
        rows = pl.ds(pl.multiple_of(step * SUBLANES, SUBLANES), SUBLANES)
        low = low_ref[rows, :]
        high = high_ref[rows, :]
        taken = jnp.zeros((SUBLANES, LANES), jnp.float32)
        for chunk in range(chunks):
            part = rows_ref[rows, chunk * LANES : (chunk + 1) * LANES]
            part = jnp.take_along_axis(part, low, axis=1, mode="promise_in_bounds")
            taken = jnp.where(high == chunk, part, taken)
        value_ref[rows, :] = taken
        return carry

    lax.fori_loop(0, tile // SUBLANES, group, 0, unroll=2)
    return value_ref[...].T[:entry_count]


def hot_rows(labels, count):
    tile = labels.shape[1]
    hot = lax.broadcasted_iota(jnp.int32, (count, tile), 0) == labels
    return hot.astype(jnp.float32).T.astype(jnp.bfloat16)


def traction_kernel(block_ref, local_ref, weight_ref, normal_ref, pressure_ref, out_ref, *scratch):
    hot = hot_rows(block_ref[...], pressure_ref.shape[0])
    cells = gather_entries(hot, pressure_ref[...], local_ref[...], *scratch)
    weighted = weight_ref[...] * cells
    tile = weighted.shape[1]
    points = out_ref.shape[0] // 3
    face_pressure = jnp.sum(weighted.reshape(points, -1, tile), axis=1)
    face_pressure = jnp.concatenate([face_pressure] * 3, axis=0)
    out_ref[...] = -(normal_ref[...] * face_pressure)


def return_kernel(part_ref, nodes_ref, shape_ref, table_ref, out_ref, *scratch):
    count, width = table_ref.shape
    table = table_ref[...]
    head = table.astype(jnp.bfloat16)
    tail = (table - head.astype(jnp.float32)).astype(jnp.bfloat16)
    hot = hot_rows(part_ref[...], count)
    owned = width // 3
    nodes = nodes_ref[...]
    entries = jnp.concatenate([nodes, nodes + owned, nodes + 2 * owned], axis=0)
    at_nodes = gather_entries(
        jnp.concatenate([hot, hot], axis=1), jnp.concatenate([head, tail], axis=0), entries, *scratch
    )
    out_ref[...] = jnp.dot(
        shape_ref[...],
        at_nodes,
        precision=lax.Precision.HIGHEST,
        preferred_element_type=jnp.float32,
    )


def face_tile(face_count):
    return math.gcd(face_count, 256)


def tile_scratch(tile, width):
    return [
        pltpu.VMEM((tile, width), jnp.float32),
        pltpu.VMEM((tile, LANES), jnp.int32),
        pltpu.VMEM((tile, LANES), jnp.int32),
        pltpu.VMEM((tile, LANES), jnp.float32),
    ]


def column_spec(rows, tile):
    return pl.BlockSpec((rows, tile), lambda step: (0, step))


def whole_spec(array):
    return pl.BlockSpec(array.shape, lambda step: (0, 0))


def stencil_traction(pressure, face_block, stencil_local, stencil_weight, area_normal):
    face_count = face_block.shape[0]
    tile = face_tile(face_count)
    flops = 2 * face_count * pressure.size
    return pl.pallas_call(
        traction_kernel,
        grid=(face_count // tile,),
        in_specs=[
            column_spec(1, tile),
            column_spec(stencil_local.shape[0], tile),
            column_spec(stencil_weight.shape[0], tile),
            column_spec(area_normal.shape[0], tile),
            whole_spec(pressure),
        ],
        out_specs=column_spec(area_normal.shape[0], tile),
        out_shape=jax.ShapeDtypeStruct(area_normal.shape, jnp.float32),
        scratch_shapes=tile_scratch(tile, pressure.shape[1]),
        cost_estimate=pl.CostEstimate(flops=flops, bytes_accessed=4 * pressure.size, transcendentals=0),
    )(face_block.reshape(1, -1), stencil_local, stencil_weight, area_normal, pressure)


def wall_points(table, face_part, face_nodes):
    face_count = face_nodes.shape[1]
    tile = face_tile(face_count)
    shapes = shape_table()
    blocks = np.zeros((3 * shapes.shape[0], 3 * shapes.shape[1]), np.float32)
    for comp in range(3):
        blocks[comp * 4 : comp * 4 + 4, comp * 8 : comp * 8 + 8] = shapes
    blocks = jnp.asarray(blocks)
    flops = 4 * face_count * table.size
    return pl.pallas_call(
        return_kernel,
        grid=(face_count // tile,),
        in_specs=[
            column_spec(1, tile),
            column_spec(face_nodes.shape[0], tile),
            whole_spec(blocks),
            whole_spec(table),
        ],
        out_specs=column_spec(blocks.shape[0], tile),
        out_shape=jax.ShapeDtypeStruct((blocks.shape[0], face_count), jnp.float32),
        scratch_shapes=tile_scratch(tile, table.shape[1]),
        cost_estimate=pl.CostEstimate(flops=flops, bytes_accessed=4 * table.size, transcendentals=0),
    )(face_part.reshape(1, -1), face_nodes, blocks, table)


def shards(
    pressure,
    face_block,
    stencil_local,
    stencil_weight,
    area_normal,
    face_part,
    face_nodes,
    stiffness,
    connect,
    halo_nodes,
    node_mass,
    displacement,
    velocity,
):
    highest = lax.Precision.HIGHEST
    gx_size = lax.axis_size("gx")
    yz_size = lax.axis_size("yz")
    devices = gx_size * yz_size
    shapes = jnp.asarray(shape_table(), dtype=jnp.float32)
    face_count = face_block.shape[0]
    capacity = max(2, 2 * face_count // devices)
    slot_total = devices * capacity
    traction = stencil_traction(pressure, face_block, stencil_local, stencil_weight, area_normal)
    target = face_part[:, 0]
    slots = target * capacity + arrival_order(target, devices)
    slot_hots = hot_pair(slots, slot_total)
    packed = spread_cols(
        jnp.concatenate([traction, face_nodes.astype(jnp.float32)], axis=0), slot_hots
    )
    load_buffer = packed[:12].reshape(12, devices, capacity)
    node_buffer = packed[12:].reshape(8, devices, capacity)
    arrived_load, arrived_nodes = (
        lax.all_to_all(load_buffer, ("gx", "yz"), split_axis=1, concat_axis=1, tiled=True),
        lax.all_to_all(node_buffer, ("gx", "yz"), split_axis=1, concat_axis=1, tiled=True),
    )
    received = arrived_load.reshape(3, 4, slot_total)
    node_ids = arrived_nodes.reshape(8 * slot_total).astype(jnp.int32)
    owned_count = displacement.shape[1]
    ghost_count = halo_nodes.shape[1]
    span = owned_count + 2 * ghost_count
    node_hots = hot_pair(node_ids, owned_count)
    load = jnp.einsum("qa,cqs->cas", shapes, received, precision=highest)
    external = spread_cols(load.reshape(3, -1), node_hots)
    element_count = connect.shape[1]
    elem_hots = hot_pair(connect.reshape(-1), span)
    halo_hots = hot_pair(halo_nodes.reshape(-1), owned_count)
    node_disp = displacement
    node_vel = velocity
    for substep in range(SUBSTEPS):
        outgoing = pick_cols(node_disp, halo_hots).reshape(3, 2, ghost_count)
        bordered = with_halo(outgoing, ((("gx", "yz"), 1),), 1)
        local_disp = jnp.concatenate([node_disp, bordered[:, 0], bordered[:, 3]], axis=1)
        element_disp = pick_cols(local_disp, elem_hots).reshape(60, element_count)
        element_force = jnp.sum(stiffness * element_disp[None], axis=1)
        spread = spread_cols(element_force.reshape(3, -1), elem_hots)
        ghost_terms = jnp.stack(
            [
                spread[:, owned_count : owned_count + ghost_count],
                spread[:, owned_count + ghost_count :],
            ],
            axis=1,
        )
        arriving = with_halo(ghost_terms, ((("gx", "yz"), 1),), 1)
        incoming = jnp.concatenate([arriving[:, 0], arriving[:, 3]], axis=1)
        internal = spread[:, :owned_count] + spread_cols(incoming, halo_hots)
        node_vel = node_vel + (external - internal) / node_mass[None, :]
        node_disp = node_disp + node_vel
    gathered = lax.all_gather(node_disp, ("gx", "yz"), axis=0, tiled=False)
    face_disp = wall_points(gathered.reshape(devices, 3 * owned_count), face_part, face_nodes)
    return (node_disp, face_disp)


def solution(mesh):
    in_specs = (
        P(("gx", "yz"), None),
        P(("gx", "yz")),
        P(None, ("gx", "yz")),
        P(None, ("gx", "yz")),
        P(None, ("gx", "yz")),
        P(("gx", "yz"), None),
        P(None, ("gx", "yz")),
        P(None, None, ("gx", "yz")),
        P(None, ("gx", "yz")),
        P(None, ("gx", "yz")),
        P(("gx", "yz")),
        P(None, ("gx", "yz")),
        P(None, ("gx", "yz")),
    )
    out_specs = (P(None, ("gx", "yz")), P(None, ("gx", "yz")))
    return jax.shard_map(shards, mesh=mesh, in_specs=in_specs, out_specs=out_specs, check_vma=False)
```

```python
import functools
import math

import jax
import jax.numpy as jnp
import numpy as np
from jax import lax
from jax.experimental import pallas as pl
from jax.experimental.pallas import tpu as pltpu
from jax.sharding import PartitionSpec as P

SUBSTEPS = 4


def shape_table():
    corner_u = [-1, 1, 1, -1, 0, 1, 0, -1]
    corner_v = [-1, -1, 1, 1, -1, 0, 1, 0]
    gauss_point = 1.0 / math.sqrt(3.0)
    points = [
        (-gauss_point, -gauss_point),
        (gauss_point, -gauss_point),
        (gauss_point, gauss_point),
        (-gauss_point, gauss_point),
    ]
    shape_values = np.zeros((4, 8), np.float32)
    for position, (coord_u, coord_v) in enumerate(points):
        for corner in range(8):
            node_u = corner_u[corner]
            node_v = corner_v[corner]
            if corner < 4:
                entry_value = (
                    0.25
                    * (1 + coord_u * node_u)
                    * (1 + coord_v * node_v)
                    * (coord_u * node_u + coord_v * node_v - 1)
                )
            elif node_u == 0:
                entry_value = 0.5 * (1 - coord_u * coord_u) * (1 + coord_v * node_v)
            else:
                entry_value = 0.5 * (1 + coord_u * node_u) * (1 - coord_v * coord_v)
            shape_values[position, corner] = entry_value
    return shape_values


def hot_pair(indices, extent):
    lanes_width = 32
    upper_count = -(-extent // lanes_width)
    upper_hot = (
        indices[None, :] // lanes_width == lax.broadcasted_iota(jnp.int32, (upper_count, 1), 0)
    ).astype(jnp.float32)
    lower_hot = (
        indices[None, :] % lanes_width == lax.broadcasted_iota(jnp.int32, (lanes_width, 1), 0)
    ).astype(jnp.float32)
    return (upper_hot, lower_hot)


def spread_cols(values, hots):
    upper_hot, lower_hot = hots
    lanes_width = lower_hot.shape[0]
    upper_count = upper_hot.shape[0]
    comps = values.shape[0]
    masked = (values[:, None, :] * lower_hot[None]).reshape(comps * lanes_width, -1)
    summed = lax.dot_general(
        masked,
        upper_hot,
        (((1,), (1,)), ((), ())),
        precision=lax.Precision.HIGHEST,
        preferred_element_type=jnp.float32,
    )
    return (
        summed.reshape(comps, lanes_width, upper_count)
        .transpose(0, 2, 1)
        .reshape(comps, upper_count * lanes_width)
    )


def arrival_order(target, devices):
    row_count = target.shape[0]
    group_rows = min(512, row_count)
    groups = row_count // group_rows
    onehot = (target[:, None] == jnp.arange(devices, dtype=jnp.int32)[None, :]).astype(jnp.bfloat16)
    onehot = onehot.reshape(groups, group_rows, devices)
    lower_ones = (
        lax.broadcasted_iota(jnp.int32, (group_rows, group_rows), 0)
        > lax.broadcasted_iota(jnp.int32, (group_rows, group_rows), 1)
    ).astype(jnp.bfloat16)
    before = jnp.einsum("ij,gjd->gid", lower_ones, onehot, preferred_element_type=jnp.float32)
    onehot_float = onehot.astype(jnp.float32)
    totals = jnp.sum(onehot_float, axis=1)
    offsets = jnp.cumsum(totals, axis=0) - totals
    placed = jnp.sum((before + offsets[:, None, :]) * onehot_float, axis=2)
    return placed.reshape(row_count).astype(jnp.int32)


LANES = 128
SUBLANES = 8


def gather_entries(hot, table, entries, rows_ref, low_ref, high_ref, value_ref):
    tile = hot.shape[0]
    entry_count = entries.shape[0]
    chunks = table.shape[1] // LANES
    rows_ref[...] = jnp.dot(hot, table, preferred_element_type=jnp.float32)
    padded = jnp.concatenate(
        [entries, jnp.zeros((LANES - entry_count, tile), jnp.int32)], axis=0
    ).T
    low_ref[...] = lax.rem(padded, LANES)
    high_ref[...] = lax.div(padded, LANES)

    def group(step, carry):
        rows = pl.ds(pl.multiple_of(step * SUBLANES, SUBLANES), SUBLANES)
        low = low_ref[rows, :]
        high = high_ref[rows, :]
        taken = jnp.zeros((SUBLANES, LANES), jnp.float32)
        for chunk in range(chunks):
            part = rows_ref[rows, chunk * LANES : (chunk + 1) * LANES]
            part = jnp.take_along_axis(part, low, axis=1, mode="promise_in_bounds")
            taken = jnp.where(high == chunk, part, taken)
        value_ref[rows, :] = taken
        return carry

    lax.fori_loop(0, tile // SUBLANES, group, 0, unroll=8)
    return value_ref[...].T[:entry_count]


def hot_rows(labels, count):
    tile = labels.shape[1]
    hot = lax.broadcasted_iota(jnp.int32, (count, tile), 0) == labels
    return hot.astype(jnp.float32).T.astype(jnp.bfloat16)


def traction_kernel(block_ref, local_ref, weight_ref, normal_ref, pressure_ref, out_ref, *scratch):
    hot = hot_rows(block_ref[...], pressure_ref.shape[0])
    cells = gather_entries(hot, pressure_ref[...], local_ref[...], *scratch)
    weighted = weight_ref[...] * cells
    tile = weighted.shape[1]
    points = out_ref.shape[0] // 3
    face_pressure = jnp.sum(weighted.reshape(points, -1, tile), axis=1)
    face_pressure = jnp.concatenate([face_pressure] * 3, axis=0)
    out_ref[...] = -(normal_ref[...] * face_pressure)


def return_kernel(part_ref, nodes_ref, shape_ref, table_ref, out_ref, *scratch):
    count, width = table_ref.shape
    table = table_ref[...]
    head = table.astype(jnp.bfloat16)
    tail = (table - head.astype(jnp.float32)).astype(jnp.bfloat16)
    hot = hot_rows(part_ref[...], count)
    owned = width // 3
    nodes = nodes_ref[...]
    entries = jnp.concatenate([nodes, nodes + owned, nodes + 2 * owned], axis=0)
    at_nodes = gather_entries(
        jnp.concatenate([hot, hot], axis=1), jnp.concatenate([head, tail], axis=0), entries, *scratch
    )
    out_ref[...] = jnp.dot(
        shape_ref[...],
        at_nodes,
        precision=lax.Precision.HIGHEST,
        preferred_element_type=jnp.float32,
    )


def face_tile(face_count):
    return math.gcd(face_count, 256)


def tile_scratch(tile, width):
    return [
        pltpu.VMEM((tile, width), jnp.float32),
        pltpu.VMEM((tile, LANES), jnp.int32),
        pltpu.VMEM((tile, LANES), jnp.int32),
        pltpu.VMEM((tile, LANES), jnp.float32),
    ]


def column_spec(rows, tile):
    return pl.BlockSpec((rows, tile), lambda step: (0, step))


def whole_spec(array):
    return pl.BlockSpec(array.shape, lambda step: (0, 0))


def stencil_traction(pressure, face_block, stencil_local, stencil_weight, area_normal):
    face_count = face_block.shape[0]
    tile = face_tile(face_count)
    flops = 2 * face_count * pressure.size
    return pl.pallas_call(
        traction_kernel,
        grid=(face_count // tile,),
        in_specs=[
            column_spec(1, tile),
            column_spec(stencil_local.shape[0], tile),
            column_spec(stencil_weight.shape[0], tile),
            column_spec(area_normal.shape[0], tile),
            whole_spec(pressure),
        ],
        out_specs=column_spec(area_normal.shape[0], tile),
        out_shape=jax.ShapeDtypeStruct(area_normal.shape, jnp.float32),
        scratch_shapes=tile_scratch(tile, pressure.shape[1]),
        cost_estimate=pl.CostEstimate(flops=flops, bytes_accessed=4 * pressure.size, transcendentals=0),
    )(face_block.reshape(1, -1), stencil_local, stencil_weight, area_normal, pressure)


def wall_points(table, face_part, face_nodes):
    face_count = face_nodes.shape[1]
    tile = face_tile(face_count)
    shapes = shape_table()
    blocks = np.zeros((3 * shapes.shape[0], 3 * shapes.shape[1]), np.float32)
    for comp in range(3):
        blocks[comp * 4 : comp * 4 + 4, comp * 8 : comp * 8 + 8] = shapes
    blocks = jnp.asarray(blocks)
    flops = 4 * face_count * table.size
    return pl.pallas_call(
        return_kernel,
        grid=(face_count // tile,),
        in_specs=[
            column_spec(1, tile),
            column_spec(face_nodes.shape[0], tile),
            whole_spec(blocks),
            whole_spec(table),
        ],
        out_specs=column_spec(blocks.shape[0], tile),
        out_shape=jax.ShapeDtypeStruct((blocks.shape[0], face_count), jnp.float32),
        scratch_shapes=tile_scratch(tile, table.shape[1]),
        cost_estimate=pl.CostEstimate(flops=flops, bytes_accessed=4 * table.size, transcendentals=0),
    )(face_part.reshape(1, -1), face_nodes, blocks, table)


def split_rows(rows):
    head = rows.astype(jnp.bfloat16)
    tail = (rows - head.astype(jnp.float32)).astype(jnp.bfloat16)
    return jnp.concatenate([head, tail], axis=0)


def spread_dot(rows, hot):
    both = lax.dot_general(
        split_rows(rows), hot, (((1,), (1,)), ((), ())), preferred_element_type=jnp.float32
    )
    return both[: rows.shape[0]] + both[rows.shape[0] :]


def solid_kernel(
    axis_sizes,
    stiff_ref,
    low_ref,
    high_ref,
    upper_ref,
    lower_ref,
    halo_low_ref,
    halo_high_ref,
    halo_upper_ref,
    halo_lower_ref,
    external_ref,
    mass_ref,
    disp_ref,
    vel_ref,
    table_ref,
    final_ref,
    send_ref,
    recv_ref,
    local_ref,
    force_ref,
    send_sem,
    recv_sem,
    wide_send_sem,
    wide_recv_sem,
):
    gx_size, yz_size = axis_sizes
    devices = gx_size * yz_size
    here = lax.axis_index("gx") * yz_size + lax.axis_index("yz")
    has_prev = here > 0
    has_next = here < devices - 1
    owned_rows = mass_ref.shape[0]
    freedom = stiff_ref.shape[0]
    nodes = freedom // 3
    padded_rows = upper_ref.shape[1]
    table_rows = owned_rows + 2
    halves = stiff_ref.shape[2] // LANES

    def place(device):
        return {"gx": lax.div(device, yz_size), "yz": lax.rem(device, yz_size)}

    def to_side(turn, side):
        return pltpu.make_async_remote_copy(
            src_ref=send_ref.at[turn, side],
            dst_ref=recv_ref.at[turn, 1 - side],
            send_sem=send_sem.at[turn, side],
            recv_sem=recv_sem.at[turn, 1 - side],
            device_id=place(here + 2 * side - 1),
            device_id_type=pl.DeviceIdType.MESH,
        )

    def swap(turn):
        @pl.when(has_prev)
        def _():
            to_side(turn, 0).start()

        @pl.when(has_next)
        def _():
            to_side(turn, 1).start()

        @pl.when(has_prev)
        def _():
            to_side(turn, 0).wait_send()
            to_side(turn, 1).wait_recv()

        @pl.when(has_next)
        def _():
            to_side(turn, 1).wait_send()
            to_side(turn, 0).wait_recv()

    blank = jnp.zeros((recv_ref.shape[0],) + recv_ref.shape[2:], jnp.float32)
    send_ref[:, 0] = blank
    send_ref[:, 1] = blank

    @pl.when(jnp.logical_not(has_prev))
    def _():
        recv_ref[:, 0] = blank

    @pl.when(jnp.logical_not(has_next))
    def _():
        recv_ref[:, 1] = blank

    def pick(row, low):
        row = jnp.broadcast_to(row, low.shape)
        return jnp.take_along_axis(row, low, axis=1, mode="promise_in_bounds")

    def substep(step, carry):
        disp, vel = carry
        turn = 2 * step
        halo_low = halo_low_ref[...]
        halo_high = halo_high_ref[...]
        for comp in range(3):
            taken = jnp.zeros(halo_low.shape, jnp.float32)
            for row in range(owned_rows):
                part = pick(disp[comp][row : row + 1], halo_low)
                taken = jnp.where(halo_high == row, part, taken)
            for side in range(2):
                send_ref[turn, side, comp : comp + 1, :] = taken[side : side + 1]
        swap(turn)
        ghosts = [recv_ref[turn, side] for side in range(2)]
        for start in range(0, low_ref.shape[0], SUBLANES):
            last = min(start + SUBLANES, freedom) - 1
            for half in range(halves):
                lanes = slice(half * LANES, (half + 1) * LANES)
                low = low_ref[start : start + SUBLANES, lanes]
                high = high_ref[start : start + SUBLANES, lanes]
                taken = jnp.zeros(low.shape, jnp.float32)
                for comp in range(start // nodes, last // nodes + 1):
                    for row in range(table_rows):
                        if row < owned_rows:
                            source = disp[comp][row : row + 1]
                        else:
                            source = ghosts[row - owned_rows][comp : comp + 1]
                        part = pick(source, low)
                        taken = jnp.where(high == comp * table_rows + row, part, taken)
                local_ref[start : start + SUBLANES, lanes] = taken
        local = local_ref[:freedom, :]
        for row in range(freedom):
            force_ref[row : row + 1, :] = jnp.sum(stiff_ref[row] * local, axis=0, keepdims=True)
        spread = jnp.zeros((3 * padded_rows, LANES), jnp.float32)
        for node in range(nodes):
            rows = [
                force_ref[comp * nodes + node : comp * nodes + node + 1, :] * upper_ref[node]
                for comp in range(3)
            ]
            spread = spread + spread_dot(jnp.concatenate(rows, axis=0), lower_ref[node])
        for comp in range(3):
            for side in range(2):
                row = comp * padded_rows + owned_rows + side
                send_ref[turn + 1, side, comp : comp + 1, :] = spread[row : row + 1]
        swap(turn + 1)
        internal = [
            spread[comp * padded_rows : comp * padded_rows + owned_rows] for comp in range(3)
        ]
        for side in range(2):
            arrived = recv_ref[turn + 1, side]
            rows = [arrived[comp : comp + 1] * halo_upper_ref[side] for comp in range(3)]
            added = spread_dot(jnp.concatenate(rows, axis=0), halo_lower_ref[side])
            internal = [
                internal[comp] + added[comp * owned_rows : (comp + 1) * owned_rows]
                for comp in range(3)
            ]
        vel = tuple(
            vel[comp] + (external_ref[comp] - internal[comp]) / mass_ref[...] for comp in range(3)
        )
        disp = tuple(disp[comp] + vel[comp] for comp in range(3))
        return disp, vel

    start = (
        tuple(disp_ref[comp] for comp in range(3)),
        tuple(vel_ref[comp] for comp in range(3)),
    )
    disp, _ = lax.fori_loop(0, SUBSTEPS, substep, start)
    for comp in range(3):
        final_ref[comp * owned_rows : (comp + 1) * owned_rows, :] = disp[comp]
    table_ref[here] = jnp.concatenate(list(disp), axis=0)

    def to_device(step):
        return pltpu.make_async_remote_copy(
            src_ref=final_ref,
            dst_ref=table_ref.at[here],
            send_sem=wide_send_sem.at[step],
            recv_sem=wide_recv_sem.at[step],
            device_id=place(lax.rem(here + step, devices)),
            device_id_type=pl.DeviceIdType.MESH,
        )

    def send_one(step, carry):
        to_device(step).start()
        return carry

    def wait_one(step, carry):
        to_device(step).wait()
        return carry

    lax.fori_loop(1, devices, send_one, 0)
    lax.fori_loop(1, devices, wait_one, 0)


def one_hot(labels, count, kind):
    shape = labels.shape[:-1] + (count, labels.shape[-1])
    return (lax.broadcasted_iota(jnp.int32, shape, len(shape) - 2) == labels[..., None, :]).astype(kind)


def solid_steps(stiffness, connect, halo_nodes, external, node_mass, displacement, velocity):
    gx_size = lax.axis_size("gx")
    yz_size = lax.axis_size("yz")
    devices = gx_size * yz_size
    owned_rows = displacement.shape[1] // LANES
    padded_rows = -(-(owned_rows + 2) // SUBLANES) * SUBLANES
    freedom, _, elements = stiffness.shape
    span = (owned_rows + 2) * LANES
    entries = jnp.concatenate([connect, connect + span, connect + 2 * span], axis=0)
    entries = jnp.pad(entries, ((0, -freedom % SUBLANES), (0, 0)))
    halo = jnp.pad(halo_nodes, ((0, -halo_nodes.shape[0] % SUBLANES), (0, 0)))
    ghosts = halo_nodes.shape[1]
    turns = 2 * SUBSTEPS
    operands = (
        stiffness,
        entries % LANES,
        entries // LANES,
        one_hot(connect // LANES, padded_rows, jnp.float32),
        one_hot(connect % LANES, LANES, jnp.bfloat16),
        halo % LANES,
        halo // LANES,
        one_hot(halo_nodes // LANES, owned_rows, jnp.float32),
        one_hot(halo_nodes % LANES, LANES, jnp.bfloat16),
        external.reshape(3, owned_rows, LANES),
        node_mass.reshape(owned_rows, LANES),
        displacement.reshape(3, owned_rows, LANES),
        velocity.reshape(3, owned_rows, LANES),
    )
    vmem = pl.BlockSpec(memory_space=pltpu.VMEM)
    return pl.pallas_call(
        functools.partial(solid_kernel, (gx_size, yz_size)),
        in_specs=[vmem] * len(operands),
        out_specs=[vmem] * 2,
        out_shape=[
            jax.ShapeDtypeStruct((devices, 3 * owned_rows, LANES), jnp.float32),
            jax.ShapeDtypeStruct((3 * owned_rows, LANES), jnp.float32),
        ],
        scratch_shapes=[
            pltpu.VMEM((turns, 2, SUBLANES, ghosts), jnp.float32),
            pltpu.VMEM((turns, 2, SUBLANES, ghosts), jnp.float32),
            pltpu.VMEM((entries.shape[0], elements), jnp.float32),
            pltpu.VMEM((entries.shape[0], elements), jnp.float32),
            pltpu.SemaphoreType.DMA((turns, 2)),
            pltpu.SemaphoreType.DMA((turns, 2)),
            pltpu.SemaphoreType.DMA((devices,)),
            pltpu.SemaphoreType.DMA((devices,)),
        ],
        compiler_params=pltpu.CompilerParams(has_side_effects=True),
        cost_estimate=pl.CostEstimate(
            flops=2 * SUBSTEPS * stiffness.size, bytes_accessed=4 * stiffness.size, transcendentals=0
        ),
    )(*operands)


def shards(
    pressure,
    face_block,
    stencil_local,
    stencil_weight,
    area_normal,
    face_part,
    face_nodes,
    stiffness,
    connect,
    halo_nodes,
    node_mass,
    displacement,
    velocity,
):
    highest = lax.Precision.HIGHEST
    gx_size = lax.axis_size("gx")
    yz_size = lax.axis_size("yz")
    devices = gx_size * yz_size
    shapes = jnp.asarray(shape_table(), dtype=jnp.float32)
    face_count = face_block.shape[0]
    capacity = max(2, 2 * face_count // devices)
    slot_total = devices * capacity
    traction = stencil_traction(pressure, face_block, stencil_local, stencil_weight, area_normal)
    target = face_part[:, 0]
    slots = target * capacity + arrival_order(target, devices)
    slot_hots = hot_pair(slots, slot_total)
    packed = spread_cols(
        jnp.concatenate([traction, face_nodes.astype(jnp.float32)], axis=0), slot_hots
    )
    load_buffer = packed[:12].reshape(12, devices, capacity)
    node_buffer = packed[12:].reshape(8, devices, capacity)
    arrived_load, arrived_nodes = (
        lax.all_to_all(load_buffer, ("gx", "yz"), split_axis=1, concat_axis=1, tiled=True),
        lax.all_to_all(node_buffer, ("gx", "yz"), split_axis=1, concat_axis=1, tiled=True),
    )
    received = arrived_load.reshape(3, 4, slot_total)
    node_ids = arrived_nodes.reshape(8 * slot_total).astype(jnp.int32)
    owned_count = displacement.shape[1]
    node_hots = hot_pair(node_ids, owned_count)
    load = jnp.einsum("qa,cqs->cas", shapes, received, precision=highest)
    external = spread_cols(load.reshape(3, -1), node_hots)
    table, final = solid_steps(
        stiffness, connect, halo_nodes, external, node_mass, displacement, velocity
    )
    node_disp = final.reshape(displacement.shape)
    face_disp = wall_points(table.reshape(devices, 3 * owned_count), face_part, face_nodes)
    return (node_disp, face_disp)


def solution(mesh):
    in_specs = (
        P(("gx", "yz"), None),
        P(("gx", "yz")),
        P(None, ("gx", "yz")),
        P(None, ("gx", "yz")),
        P(None, ("gx", "yz")),
        P(("gx", "yz"), None),
        P(None, ("gx", "yz")),
        P(None, None, ("gx", "yz")),
        P(None, ("gx", "yz")),
        P(None, ("gx", "yz")),
        P(("gx", "yz")),
        P(None, ("gx", "yz")),
        P(None, ("gx", "yz")),
    )
    out_specs = (P(None, ("gx", "yz")), P(None, ("gx", "yz")))
    return jax.shard_map(shards, mesh=mesh, in_specs=in_specs, out_specs=out_specs, check_vma=False)
```

```python
import functools
import math

import jax
import jax.numpy as jnp
import numpy as np
from jax import lax
from jax.experimental import pallas as pl
from jax.experimental.pallas import tpu as pltpu
from jax.sharding import PartitionSpec as P

SUBSTEPS = 4


def shape_table():
    corner_u = [-1, 1, 1, -1, 0, 1, 0, -1]
    corner_v = [-1, -1, 1, 1, -1, 0, 1, 0]
    gauss_point = 1.0 / math.sqrt(3.0)
    points = [
        (-gauss_point, -gauss_point),
        (gauss_point, -gauss_point),
        (gauss_point, gauss_point),
        (-gauss_point, gauss_point),
    ]
    shape_values = np.zeros((4, 8), np.float32)
    for position, (coord_u, coord_v) in enumerate(points):
        for corner in range(8):
            node_u = corner_u[corner]
            node_v = corner_v[corner]
            if corner < 4:
                entry_value = (
                    0.25
                    * (1 + coord_u * node_u)
                    * (1 + coord_v * node_v)
                    * (coord_u * node_u + coord_v * node_v - 1)
                )
            elif node_u == 0:
                entry_value = 0.5 * (1 - coord_u * coord_u) * (1 + coord_v * node_v)
            else:
                entry_value = 0.5 * (1 + coord_u * node_u) * (1 - coord_v * coord_v)
            shape_values[position, corner] = entry_value
    return shape_values


def hot_pair(indices, extent):
    lanes_width = 32
    upper_count = -(-extent // lanes_width)
    upper_hot = (
        indices[None, :] // lanes_width == lax.broadcasted_iota(jnp.int32, (upper_count, 1), 0)
    ).astype(jnp.float32)
    lower_hot = (
        indices[None, :] % lanes_width == lax.broadcasted_iota(jnp.int32, (lanes_width, 1), 0)
    ).astype(jnp.float32)
    return (upper_hot, lower_hot)


def spread_cols(values, hots):
    upper_hot, lower_hot = hots
    lanes_width = lower_hot.shape[0]
    upper_count = upper_hot.shape[0]
    comps = values.shape[0]
    head = lax.reduce_precision(values, 8, 7)
    tail = lax.reduce_precision(values - head, 8, 7)
    parts = jnp.concatenate([head, tail], axis=0).astype(jnp.bfloat16)
    masked = (parts[:, None, :] * lower_hot.astype(jnp.bfloat16)[None]).reshape(
        2 * comps * lanes_width, -1
    )
    summed = lax.dot_general(
        masked,
        upper_hot.astype(jnp.bfloat16),
        (((1,), (1,)), ((), ())),
        preferred_element_type=jnp.float32,
    )
    summed = summed[: comps * lanes_width] + summed[comps * lanes_width :]
    return (
        summed.reshape(comps, lanes_width, upper_count)
        .transpose(0, 2, 1)
        .reshape(comps, upper_count * lanes_width)
    )


def arrival_order(target, devices):
    row_count = target.shape[0]
    group_rows = min(512, row_count)
    groups = row_count // group_rows
    onehot = (target[:, None] == jnp.arange(devices, dtype=jnp.int32)[None, :]).astype(jnp.bfloat16)
    onehot = onehot.reshape(groups, group_rows, devices)
    lower_ones = (
        lax.broadcasted_iota(jnp.int32, (group_rows, group_rows), 0)
        > lax.broadcasted_iota(jnp.int32, (group_rows, group_rows), 1)
    ).astype(jnp.bfloat16)
    before = jnp.einsum("ij,gjd->gid", lower_ones, onehot, preferred_element_type=jnp.float32)
    onehot_float = onehot.astype(jnp.float32)
    totals = jnp.sum(onehot_float, axis=1)
    offsets = jnp.cumsum(totals, axis=0) - totals
    placed = jnp.sum((before + offsets[:, None, :]) * onehot_float, axis=2)
    return placed.reshape(row_count).astype(jnp.int32)


LANES = 128
SUBLANES = 8


def gather_entries(hot, table, entries, rows_ref, low_ref, high_ref, value_ref):
    tile = hot.shape[0]
    entry_count = entries.shape[0]
    chunks = table.shape[1] // LANES
    padded = jnp.concatenate(
        [entries, jnp.zeros((LANES - entry_count, tile), jnp.int32)], axis=0
    ).T
    low_ref[...] = lax.rem(padded, LANES)
    high_ref[...] = lax.div(padded, LANES)
    sub = math.gcd(tile, LANES)
    for first in range(0, tile, sub):
        rows_ref[first : first + sub, :] = jnp.dot(
            hot[first : first + sub], table, preferred_element_type=jnp.float32
        )
        for start in range(first, first + sub, SUBLANES):
            rows = slice(start, start + SUBLANES)
            low = low_ref[rows, :]
            high = high_ref[rows, :]
            taken = jnp.zeros((SUBLANES, LANES), jnp.float32)
            for chunk in range(chunks):
                part = rows_ref[rows, chunk * LANES : (chunk + 1) * LANES]
                part = jnp.take_along_axis(part, low, axis=1, mode="promise_in_bounds")
                taken = jnp.where(high == chunk, part, taken)
            value_ref[rows, :] = taken
    return value_ref[...].T[:entry_count]


def hot_rows(labels, count):
    tile = labels.shape[1]
    hot = lax.broadcasted_iota(jnp.int32, (count, tile), 0) == labels
    return hot.astype(jnp.float32).T.astype(jnp.bfloat16)


def traction_kernel(block_ref, local_ref, weight_ref, normal_ref, pressure_ref, out_ref, *scratch):
    hot = hot_rows(block_ref[...], pressure_ref.shape[0])
    cells = gather_entries(hot, pressure_ref[...], local_ref[...], *scratch)
    weighted = weight_ref[...] * cells
    tile = weighted.shape[1]
    points = out_ref.shape[0] // 3
    face_pressure = jnp.sum(weighted.reshape(points, -1, tile), axis=1)
    face_pressure = jnp.concatenate([face_pressure] * 3, axis=0)
    out_ref[...] = -(normal_ref[...] * face_pressure)


def return_kernel(part_ref, nodes_ref, shape_ref, table_ref, out_ref, *scratch):
    count, width = table_ref.shape
    table = table_ref[...]
    head = table.astype(jnp.bfloat16)
    tail = (table - head.astype(jnp.float32)).astype(jnp.bfloat16)
    hot = hot_rows(part_ref[...], count)
    owned = width // 3
    nodes = nodes_ref[...]
    entries = jnp.concatenate([nodes, nodes + owned, nodes + 2 * owned], axis=0)
    at_nodes = gather_entries(
        jnp.concatenate([hot, hot], axis=1), jnp.concatenate([head, tail], axis=0), entries, *scratch
    )
    out_ref[...] = jnp.dot(
        shape_ref[...],
        at_nodes,
        precision=lax.Precision.HIGHEST,
        preferred_element_type=jnp.float32,
    )


def face_tile(face_count):
    return math.gcd(face_count, 512)


def tile_scratch(tile, width):
    return [
        pltpu.VMEM((tile, width), jnp.float32),
        pltpu.VMEM((tile, LANES), jnp.int32),
        pltpu.VMEM((tile, LANES), jnp.int32),
        pltpu.VMEM((tile, LANES), jnp.float32),
    ]


def column_spec(rows, tile):
    return pl.BlockSpec((rows, tile), lambda step: (0, step))


def whole_spec(array):
    return pl.BlockSpec(array.shape, lambda step: (0, 0))


def stencil_traction(pressure, face_block, stencil_local, stencil_weight, area_normal):
    face_count = face_block.shape[0]
    tile = face_tile(face_count)
    flops = 2 * face_count * pressure.size
    return pl.pallas_call(
        traction_kernel,
        grid=(face_count // tile,),
        in_specs=[
            column_spec(1, tile),
            column_spec(stencil_local.shape[0], tile),
            column_spec(stencil_weight.shape[0], tile),
            column_spec(area_normal.shape[0], tile),
            whole_spec(pressure),
        ],
        out_specs=column_spec(area_normal.shape[0], tile),
        out_shape=jax.ShapeDtypeStruct(area_normal.shape, jnp.float32),
        scratch_shapes=tile_scratch(tile, pressure.shape[1]),
        cost_estimate=pl.CostEstimate(flops=flops, bytes_accessed=4 * pressure.size, transcendentals=0),
    )(face_block.reshape(1, -1), stencil_local, stencil_weight, area_normal, pressure)


def wall_points(table, face_part, face_nodes):
    face_count = face_nodes.shape[1]
    tile = face_tile(face_count)
    shapes = shape_table()
    blocks = np.zeros((3 * shapes.shape[0], 3 * shapes.shape[1]), np.float32)
    for comp in range(3):
        blocks[comp * 4 : comp * 4 + 4, comp * 8 : comp * 8 + 8] = shapes
    blocks = jnp.asarray(blocks)
    flops = 4 * face_count * table.size
    return pl.pallas_call(
        return_kernel,
        grid=(face_count // tile,),
        in_specs=[
            column_spec(1, tile),
            column_spec(face_nodes.shape[0], tile),
            whole_spec(blocks),
            whole_spec(table),
        ],
        out_specs=column_spec(blocks.shape[0], tile),
        out_shape=jax.ShapeDtypeStruct((blocks.shape[0], face_count), jnp.float32),
        scratch_shapes=tile_scratch(tile, table.shape[1]),
        cost_estimate=pl.CostEstimate(flops=flops, bytes_accessed=4 * table.size, transcendentals=0),
    )(face_part.reshape(1, -1), face_nodes, blocks, table)


def split_rows(rows):
    head = rows.astype(jnp.bfloat16)
    tail = (rows - head.astype(jnp.float32)).astype(jnp.bfloat16)
    return jnp.concatenate([head, tail], axis=0)


def spread_dot(rows, hot):
    both = lax.dot_general(
        split_rows(rows), hot, (((1,), (1,)), ((), ())), preferred_element_type=jnp.float32
    )
    return both[: rows.shape[0]] + both[rows.shape[0] :]


def solid_kernel(
    axis_sizes,
    stiff_ref,
    low_ref,
    high_ref,
    upper_ref,
    lower_ref,
    halo_low_ref,
    halo_high_ref,
    halo_upper_ref,
    halo_lower_ref,
    external_ref,
    mass_ref,
    disp_ref,
    vel_ref,
    table_ref,
    final_ref,
    send_ref,
    recv_ref,
    local_ref,
    force_ref,
    send_sem,
    recv_sem,
    wide_send_sem,
    wide_recv_sem,
):
    gx_size, yz_size = axis_sizes
    devices = gx_size * yz_size
    here = lax.axis_index("gx") * yz_size + lax.axis_index("yz")
    has_prev = here > 0
    has_next = here < devices - 1
    owned_rows = mass_ref.shape[0]
    freedom = stiff_ref.shape[0]
    nodes = freedom // 3
    padded_rows = upper_ref.shape[1]
    table_rows = owned_rows + 2
    halves = stiff_ref.shape[2] // LANES

    def place(device):
        return {"gx": lax.div(device, yz_size), "yz": lax.rem(device, yz_size)}

    def to_side(turn, side):
        return pltpu.make_async_remote_copy(
            src_ref=send_ref.at[turn, side],
            dst_ref=recv_ref.at[turn, 1 - side],
            send_sem=send_sem.at[turn, side],
            recv_sem=recv_sem.at[turn, 1 - side],
            device_id=place(here + 2 * side - 1),
            device_id_type=pl.DeviceIdType.MESH,
        )

    def swap(turn):
        @pl.when(has_prev)
        def _():
            to_side(turn, 0).start()

        @pl.when(has_next)
        def _():
            to_side(turn, 1).start()

        @pl.when(has_prev)
        def _():
            to_side(turn, 0).wait_send()
            to_side(turn, 1).wait_recv()

        @pl.when(has_next)
        def _():
            to_side(turn, 1).wait_send()
            to_side(turn, 0).wait_recv()

    blank = jnp.zeros((recv_ref.shape[0],) + recv_ref.shape[2:], jnp.float32)
    send_ref[:, 0] = blank
    send_ref[:, 1] = blank

    @pl.when(jnp.logical_not(has_prev))
    def _():
        recv_ref[:, 0] = blank

    @pl.when(jnp.logical_not(has_next))
    def _():
        recv_ref[:, 1] = blank

    def pick(row, low):
        row = jnp.broadcast_to(row, low.shape)
        return jnp.take_along_axis(row, low, axis=1, mode="promise_in_bounds")

    def substep(step, carry):
        disp, vel = carry
        turn = 2 * step
        halo_low = halo_low_ref[...]
        halo_high = halo_high_ref[...]
        for comp in range(3):
            taken = jnp.zeros(halo_low.shape, jnp.float32)
            for row in range(owned_rows):
                part = pick(disp[comp][row : row + 1], halo_low)
                taken = jnp.where(halo_high == row, part, taken)
            for side in range(2):
                send_ref[turn, side, comp : comp + 1, :] = taken[side : side + 1]
        swap(turn)
        ghosts = [recv_ref[turn, side] for side in range(2)]
        for start in range(0, low_ref.shape[0], SUBLANES):
            last = min(start + SUBLANES, freedom) - 1
            for half in range(halves):
                lanes = slice(half * LANES, (half + 1) * LANES)
                low = low_ref[start : start + SUBLANES, lanes]
                high = high_ref[start : start + SUBLANES, lanes]
                taken = jnp.zeros(low.shape, jnp.float32)
                for comp in range(start // nodes, last // nodes + 1):
                    for row in range(table_rows):
                        if row < owned_rows:
                            source = disp[comp][row : row + 1]
                        else:
                            source = ghosts[row - owned_rows][comp : comp + 1]
                        part = pick(source, low)
                        taken = jnp.where(high == comp * table_rows + row, part, taken)
                local_ref[start : start + SUBLANES, lanes] = taken
        local = local_ref[:freedom, :]
        for row in range(freedom):
            force_ref[row : row + 1, :] = jnp.sum(stiff_ref[row] * local, axis=0, keepdims=True)
        spread = jnp.zeros((3 * padded_rows, LANES), jnp.float32)
        for node in range(nodes):
            rows = [
                force_ref[comp * nodes + node : comp * nodes + node + 1, :] * upper_ref[node]
                for comp in range(3)
            ]
            spread = spread + spread_dot(jnp.concatenate(rows, axis=0), lower_ref[node])
        for comp in range(3):
            for side in range(2):
                row = comp * padded_rows + owned_rows + side
                send_ref[turn + 1, side, comp : comp + 1, :] = spread[row : row + 1]
        swap(turn + 1)
        internal = [
            spread[comp * padded_rows : comp * padded_rows + owned_rows] for comp in range(3)
        ]
        for side in range(2):
            arrived = recv_ref[turn + 1, side]
            rows = [arrived[comp : comp + 1] * halo_upper_ref[side] for comp in range(3)]
            added = spread_dot(jnp.concatenate(rows, axis=0), halo_lower_ref[side])
            internal = [
                internal[comp] + added[comp * owned_rows : (comp + 1) * owned_rows]
                for comp in range(3)
            ]
        vel = tuple(
            vel[comp] + (external_ref[comp] - internal[comp]) / mass_ref[...] for comp in range(3)
        )
        disp = tuple(disp[comp] + vel[comp] for comp in range(3))
        return disp, vel

    start = (
        tuple(disp_ref[comp] for comp in range(3)),
        tuple(vel_ref[comp] for comp in range(3)),
    )
    disp, _ = lax.fori_loop(0, SUBSTEPS, substep, start)
    for comp in range(3):
        final_ref[comp * owned_rows : (comp + 1) * owned_rows, :] = disp[comp]
    table_ref[here] = jnp.concatenate(list(disp), axis=0)

    def to_device(step):
        return pltpu.make_async_remote_copy(
            src_ref=final_ref,
            dst_ref=table_ref.at[here],
            send_sem=wide_send_sem.at[step],
            recv_sem=wide_recv_sem.at[step],
            device_id=place(lax.rem(here + step, devices)),
            device_id_type=pl.DeviceIdType.MESH,
        )

    def send_one(step, carry):
        to_device(step).start()
        return carry

    def wait_one(step, carry):
        to_device(step).wait()
        return carry

    lax.fori_loop(1, devices, send_one, 0)
    lax.fori_loop(1, devices, wait_one, 0)


def one_hot(labels, count, kind):
    shape = labels.shape[:-1] + (count, labels.shape[-1])
    return (lax.broadcasted_iota(jnp.int32, shape, len(shape) - 2) == labels[..., None, :]).astype(kind)


def solid_steps(stiffness, connect, halo_nodes, external, node_mass, displacement, velocity):
    gx_size = lax.axis_size("gx")
    yz_size = lax.axis_size("yz")
    devices = gx_size * yz_size
    owned_rows = displacement.shape[1] // LANES
    padded_rows = -(-(owned_rows + 2) // SUBLANES) * SUBLANES
    freedom, _, elements = stiffness.shape
    span = (owned_rows + 2) * LANES
    entries = jnp.concatenate([connect, connect + span, connect + 2 * span], axis=0)
    entries = jnp.pad(entries, ((0, -freedom % SUBLANES), (0, 0)))
    halo = jnp.pad(halo_nodes, ((0, -halo_nodes.shape[0] % SUBLANES), (0, 0)))
    ghosts = halo_nodes.shape[1]
    turns = 2 * SUBSTEPS
    operands = (
        stiffness,
        entries % LANES,
        entries // LANES,
        one_hot(connect // LANES, padded_rows, jnp.float32),
        one_hot(connect % LANES, LANES, jnp.bfloat16),
        halo % LANES,
        halo // LANES,
        one_hot(halo_nodes // LANES, owned_rows, jnp.float32),
        one_hot(halo_nodes % LANES, LANES, jnp.bfloat16),
        external.reshape(3, owned_rows, LANES),
        node_mass.reshape(owned_rows, LANES),
        displacement.reshape(3, owned_rows, LANES),
        velocity.reshape(3, owned_rows, LANES),
    )
    vmem = pl.BlockSpec(memory_space=pltpu.VMEM)
    return pl.pallas_call(
        functools.partial(solid_kernel, (gx_size, yz_size)),
        in_specs=[vmem] * len(operands),
        out_specs=[vmem] * 2,
        out_shape=[
            jax.ShapeDtypeStruct((devices, 3 * owned_rows, LANES), jnp.float32),
            jax.ShapeDtypeStruct((3 * owned_rows, LANES), jnp.float32),
        ],
        scratch_shapes=[
            pltpu.VMEM((turns, 2, SUBLANES, ghosts), jnp.float32),
            pltpu.VMEM((turns, 2, SUBLANES, ghosts), jnp.float32),
            pltpu.VMEM((entries.shape[0], elements), jnp.float32),
            pltpu.VMEM((entries.shape[0], elements), jnp.float32),
            pltpu.SemaphoreType.DMA((turns, 2)),
            pltpu.SemaphoreType.DMA((turns, 2)),
            pltpu.SemaphoreType.DMA((devices,)),
            pltpu.SemaphoreType.DMA((devices,)),
        ],
        compiler_params=pltpu.CompilerParams(has_side_effects=True),
        cost_estimate=pl.CostEstimate(
            flops=2 * SUBSTEPS * stiffness.size, bytes_accessed=4 * stiffness.size, transcendentals=0
        ),
    )(*operands)


def shards(
    pressure,
    face_block,
    stencil_local,
    stencil_weight,
    area_normal,
    face_part,
    face_nodes,
    stiffness,
    connect,
    halo_nodes,
    node_mass,
    displacement,
    velocity,
):
    highest = lax.Precision.HIGHEST
    gx_size = lax.axis_size("gx")
    yz_size = lax.axis_size("yz")
    devices = gx_size * yz_size
    shapes = jnp.asarray(shape_table(), dtype=jnp.float32)
    face_count = face_block.shape[0]
    capacity = max(2, 2 * face_count // devices)
    slot_total = devices * capacity
    traction = stencil_traction(pressure, face_block, stencil_local, stencil_weight, area_normal)
    target = face_part[:, 0]
    slots = target * capacity + arrival_order(target, devices)
    slot_hots = hot_pair(slots, slot_total)
    packed = spread_cols(
        jnp.concatenate([traction, face_nodes.astype(jnp.float32)], axis=0), slot_hots
    )
    load_buffer = packed[:12].reshape(12, devices, capacity)
    node_buffer = packed[12:].reshape(8, devices, capacity)
    arrived_load, arrived_nodes = (
        lax.all_to_all(load_buffer, ("gx", "yz"), split_axis=1, concat_axis=1, tiled=True),
        lax.all_to_all(node_buffer, ("gx", "yz"), split_axis=1, concat_axis=1, tiled=True),
    )
    received = arrived_load.reshape(3, 4, slot_total)
    node_ids = arrived_nodes.reshape(8 * slot_total).astype(jnp.int32)
    owned_count = displacement.shape[1]
    node_hots = hot_pair(node_ids, owned_count)
    load = jnp.einsum("qa,cqs->cas", shapes, received, precision=highest)
    external = spread_cols(load.reshape(3, -1), node_hots)
    table, final = solid_steps(
        stiffness, connect, halo_nodes, external, node_mass, displacement, velocity
    )
    node_disp = final.reshape(displacement.shape)
    face_disp = wall_points(table.reshape(devices, 3 * owned_count), face_part, face_nodes)
    return (node_disp, face_disp)


def solution(mesh):
    in_specs = (
        P(("gx", "yz"), None),
        P(("gx", "yz")),
        P(None, ("gx", "yz")),
        P(None, ("gx", "yz")),
        P(None, ("gx", "yz")),
        P(("gx", "yz"), None),
        P(None, ("gx", "yz")),
        P(None, None, ("gx", "yz")),
        P(None, ("gx", "yz")),
        P(None, ("gx", "yz")),
        P(("gx", "yz")),
        P(None, ("gx", "yz")),
        P(None, ("gx", "yz")),
    )
    out_specs = (P(None, ("gx", "yz")), P(None, ("gx", "yz")))
    return jax.shard_map(shards, mesh=mesh, in_specs=in_specs, out_specs=out_specs, check_vma=False)
```
